32 devices in a mesh: dp: 2 (over z, core), ep: 16 (over x, y).
Axes of the slice: x: 4, y: 4, z: 1, core: 2. Of those that a mesh axis runs over, the one named last changes fastest.
The devices are a block of a 4x4x8 slice.
Arguments:
- x: bfloat16 [2, 16, 256, 3584], P('dp', 'ep'), parts along dimension 0
- expert: int32 [2, 16, 256, 8], P('dp', 'ep'), parts along dimension 0
- slot: int32 [2, 16, 256, 8], P('dp', 'ep'), parts along dimension 0
- gate: float32 [2, 16, 256, 8], P('dp', 'ep'), parts along dimension 0
- w_gate: bfloat16 [48, 3584, 2048], P('ep')
- w_up: bfloat16 [48, 3584, 2048], P('ep')
- w_down: bfloat16 [48, 2048, 3584], P('ep')
- s_gate: bfloat16 [3584, 2048], replicated
- s_up: bfloat16 [3584, 2048], replicated
- s_down: bfloat16 [2048, 3584], replicated
Outputs:
- y: bfloat16 [2, 16, 256, 3584], P('dp', 'ep'), parts along dimension 0
There are 2 independent parts. The reference program is written for one: setup_inputs(seed, part) draws one part's arguments, and reference() takes and returns one part's arrays. A program takes and returns all parts, laid end to end along the dimension named above; an argument that names none is the same for every part.
All inputs are finite; a program needn't handle non-finite values.
Results may differ from the reference program's by a relative error of at most 0.009.
Values are sent between devices in bfloat16 or wider.
A program may use at most 768 MiB of HBM per device.

```python
import jax
import jax.numpy as jnp

MEMBERS = 16
TOKENS = 256
D = 3584
FF = 2048
TOP = 8
EXPERTS = 48
SHARED_FF = 2048
SLOTS = 5 * TOKENS * TOP // (4 * EXPERTS)


def setup_inputs(seed: int = 0, part: int = 0) -> dict:
    own, k1, k2, k3, k4, k5, k6 = jax.random.split(jax.random.key(seed), 7)
    kx, ke, kl, kg = jax.random.split(jax.random.fold_in(own, part), 4)
    devices = (1, MEMBERS)
    place = jax.random.permutation(kl, jnp.arange(EXPERTS, dtype=jnp.uint32))
    slow = ((EXPERTS + (9 * place) % EXPERTS) << ((9 * place) // EXPERTS)) // EXPERTS
    wait = (jax.random.bits(ke, (*devices, TOKENS, EXPERTS), jnp.uint32) >> 10) * slow
    expert = jnp.argsort(wait, axis=-1)[..., :TOP].astype(jnp.int32)
    chosen = jax.nn.one_hot(expert, EXPERTS, dtype=jnp.int32)
    in_line = jnp.cumsum(chosen.reshape(*devices, TOKENS * TOP, EXPERTS), axis=2) - 1
    slot = jnp.sum(in_line.reshape(chosen.shape) * chosen, axis=-1)

    def one(key, rows, columns):
        return (jax.random.normal(key, (rows, columns), jnp.float32) * rows**-0.5).astype(jnp.bfloat16)

    def weights(key, rows, columns):
        return jax.lax.map(lambda k: one(k, rows, columns), jax.random.split(key, EXPERTS))

    return {
        "x": jax.random.normal(kx, (*devices, TOKENS, D), jnp.float32).astype(jnp.bfloat16),
        "expert": expert,
        "slot": slot,
        "gate": jax.nn.softmax(jax.random.normal(kg, expert.shape, jnp.float32)),
        "w_gate": weights(k1, D, FF),
        "w_up": weights(k2, D, FF),
        "w_down": weights(k3, FF, D),
        "s_gate": one(k4, D, SHARED_FF),
        "s_up": one(k5, D, SHARED_FF),
        "s_down": one(k6, SHARED_FF, D),
    }


def einsum(form, a, b):
    return jnp.einsum(form, a.astype(jnp.float32), b.astype(jnp.float32))


def for_all(x, s_gate, s_up, s_down):
    h = jax.nn.silu(einsum("...d,df->...f", x, s_gate)) * einsum("...d,df->...f", x, s_up)
    return einsum("...f,fd->...d", h.astype(jnp.bfloat16), s_down)


def reference(x, expert, slot, gate, w_gate, w_up, w_down, s_gate, s_up, s_down):
    to_expert = jax.nn.one_hot(expert, EXPERTS, dtype=jnp.bfloat16)
    to_slot = jax.nn.one_hot(slot, SLOTS, dtype=jnp.bfloat16)
    weighted = to_expert * gate[..., None].astype(jnp.bfloat16)
    dispatch = einsum("abtke,abtkc->abtec", to_expert, to_slot).astype(jnp.bfloat16)
    combine = einsum("abtke,abtkc->abtec", weighted, to_slot).astype(jnp.bfloat16)
    z = einsum("abtec,abtd->aebcd", dispatch, x).astype(jnp.bfloat16)
    h = jax.nn.silu(einsum("aebcd,edf->aebcf", z, w_gate))
    h = (h * einsum("aebcd,edf->aebcf", z, w_up)).astype(jnp.bfloat16)
    out = einsum("aebcf,efd->aebcd", h, w_down).astype(jnp.bfloat16)
    y = einsum("abtec,aebcd->abtd", combine, out)
    return (y + for_all(x, s_gate, s_up, s_down)).astype(jnp.bfloat16)
```

```python
import functools
import math

import jax
import jax.numpy as jnp
from jax import lax
from jax.experimental import pallas as pl
from jax.experimental.pallas import tpu as pltpu
from jax.sharding import PartitionSpec as P

MESH = pl.DeviceIdType.MESH
F32, BF16 = jnp.float32, jnp.bfloat16
ANY = pl.BlockSpec(memory_space=pl.ANY)
DIRS = (1, -1)
HALF = 256
CHUNK = 2 * HALF
WINDOW = 80


def place(side):
    me = lax.axis_index("ep")
    x, y = me // side, me % side

    def at(dx, dy):
        return {"ep": (x + dx + side) % side * side + (y + dy + side) % side}

    def first(half, d):
        return at(d, 0) if half == 0 else at(0, d)

    def second(half, d):
        return at(0, d) if half == 0 else at(d, 0)

    return me, ((y, x), (x, y)), first, second


def meet(side):
    _, _, first, second = place(side)
    barrier = pltpu.get_barrier_semaphore()
    for d in DIRS:
        pl.semaphore_signal(barrier, inc=1, device_id=first(0, d), device_id_type=MESH)
        pl.semaphore_signal(barrier, inc=1, device_id=second(0, d), device_id_type=MESH)
    pl.semaphore_wait(barrier, 4)


def window_of(s, slots):
    return pl.multiple_of(slots * s // 16 * 16, 16)


def up_kernel(side, slots, x_ref, meta_ref, wg_ref, wu_ref, sg_ref, su_ref,
              h_ref, hs_ref, cmb_ref, g_ref, gm_ref,
              acc, z, xs, xown, wbuf, sel, mst, hst, cst,
              snd, rcv, msnd, mrcv, wsem, xsem, osem, hsem, csem, lsem):
    me, pos, first, second = place(side)
    n = side * side
    tokens, depth = x_ref.shape
    width = wg_ref.shape[2]
    chunks = depth // CHUNK
    local = wg_ref.shape[0]
    rows = slots * n

    def gather(c, step, half, di):
        d = DIRS[di]
        o, i = pos[half]
        k = step * 4 + half * 2 + di
        part = pl.ds(0 if di == 0 else tokens // 2, tokens // 2)
        pair = pl.ds(0 if di == 0 else side // 2, side // 2)
        if step == 0:
            src = xown.at[:, pl.ds(pl.multiple_of(c * CHUNK + half * HALF, HALF), HALF)]
            dst = g_ref.at[c, half, o, i]
        elif step == 1:
            src = dst = g_ref.at[c, half, o, (i - d + side) % side, part]
        elif step == 2:
            src = dst = g_ref.at[c, half, o]
        else:
            src = dst = g_ref.at[c, half, (o - d + side) % side, pair]
        return pltpu.make_async_remote_copy(
            src_ref=src, dst_ref=dst, send_sem=snd.at[c, k], recv_sem=rcv.at[c, k],
            device_id=(first if step < 2 else second)(half, d), device_id_type=MESH)

    def each(c, step, act):
        for half in range(2):
            for di in range(2):
                act(gather(c, step, half, di))

    def start(c, step):
        each(c, step, lambda cp: cp.start())

    def landed(c, step):
        each(c, step, lambda cp: cp.wait_recv())

    y, x = pos[0]

    def meta(k):
        di = k % 2
        d = DIRS[di]
        if k < 2:
            src, dst, to = meta_ref, gm_ref.at[y, x], first(0, d)
        elif k == 2:
            src = dst = gm_ref.at[y, (x - 1 + side) % side]
            to = first(0, 1)
        elif k < 5:
            src = dst = gm_ref.at[y]
            to = second(0, DIRS[k - 3])
        else:
            src = dst = gm_ref.at[(y - 1 + side) % side]
            to = second(0, 1)
        return pltpu.make_async_remote_copy(
            src_ref=src, dst_ref=dst, send_sem=msnd.at[k], recv_sem=mrcv.at[k],
            device_id=to, device_id_type=MESH)

    def own(c, half):
        o, i = pos[half]
        return pltpu.make_async_copy(
            xown.at[:, pl.ds(pl.multiple_of(c * CHUNK + half * HALF, HALF), HALF)],
            g_ref.at[c, half, o, i], osem.at[c, half])

    def shared_tile(q):
        ref = (sg_ref, su_ref)[q % 2]
        return pltpu.make_async_copy(ref.at[pl.ds(q // 2 * CHUNK, CHUNK)], wbuf.at[q % 3], wsem.at[q % 3])

    def tile(c, j):
        ref = (wg_ref, wu_ref)[j % 2]
        return pltpu.make_async_copy(
            ref.at[j // 2, pl.ds(pl.multiple_of(c * CHUNK, CHUNK), CHUNK)], wbuf.at[j % 3], wsem.at[j % 3])

    load_x = pltpu.make_async_copy(x_ref, xown, lsem.at[0])
    load_x.start()
    keep_meta = pltpu.make_async_copy(meta_ref, mst.at[y, x], lsem.at[1])
    keep_meta.start()
    for q in range(3):
        shared_tile(q).start()
    meet(side)
    load_x.wait()
    keep_meta.wait()
    put_meta = pltpu.make_async_copy(mst.at[y, x], gm_ref.at[y, x], lsem.at[1])
    put_meta.start()

    for k in range(2):
        meta(k).start()
    start(0, 0)

    @pl.loop(0, chunks)
    def _(c):
        for half in range(2):
            own(c, half).start()

    def shared_piece(kc):
        for m in range(2):
            q = kc * 2 + m
            shared_tile(q).wait()

            @pl.loop(0, width // HALF)
            def _(nb):
                cols = pl.ds(pl.multiple_of(nb * HALF, HALF), HALF)
                into = pl.ds(pl.multiple_of(m * width + nb * HALF, HALF), HALF)
                r = jnp.dot(xown[:, kc * CHUNK:(kc + 1) * CHUNK], wbuf[q % 3, :, cols], preferred_element_type=F32)
                if kc > 0:
                    r = acc[0, :tokens, into] + r
                acc[0, :tokens, into] = r

            if q + 3 < 2 * chunks:
                shared_tile(q + 3).start()

    def finish(e, m_rows, dst_ref):
        def put(b, slot):
            cols = pl.ds(pl.multiple_of(b * HALF, HALF), HALF)
            return pltpu.make_async_copy(hst.at[slot, pl.ds(0, m_rows)], dst_ref.at[:, cols], hsem.at[slot])

        for b in range(width // HALF):
            slot = b % 2
            if b >= 2:
                put(b - 2, slot).wait()
            cols = pl.ds(b * HALF, HALF)
            ups = pl.ds(width + b * HALF, HALF)
            gate = acc[e, :m_rows, cols]
            hst[slot, :m_rows] = (jax.nn.silu(gate) * acc[e, :m_rows, ups]).astype(BF16)
            put(b, slot).start()
        for b in range(width // HALF - 2, width // HALF):
            put(b, b % 2).wait()

    for t in range(6):
        if t > 0:
            start(t, 0)
            landed(t - 1, 0)
            start(t - 1, 1)
        if t == 1:
            for k in range(2):
                meta(k).wait_recv()
            meta(2).start()
        if t >= 2:
            landed(t - 2, 1)
            for half in range(2):
                own(t - 2, half).wait()
            start(t - 2, 2)
        if t == 2:
            put_meta.wait()
            meta(2).wait_recv()
            meta(3).start()
            meta(4).start()
        if t == 3:
            meta(3).wait_recv()
            meta(4).wait_recv()
            meta(5).start()
        if t >= 4:
            landed(t - 4, 2)
            start(t - 4, 3)
        shared_piece(t)
        if t == 4:
            meta(5).wait_recv()
            load_m = pltpu.make_async_copy(gm_ref, mst, lsem.at[1])
            load_m.start()
            load_m.wait()

            @pl.loop(0, n)
            def _(s):
                r = lax.broadcasted_iota(jnp.int32, (tokens, 1), 0)
                e = (r >= WINDOW).astype(jnp.int32) + (r >= 2 * WINDOW).astype(jnp.int32)
                off = (r - e * WINDOW + window_of(s, slots) - slots * s).astype(F32)
                expert = jnp.where(r < local * WINDOW, me * local + e, -1).astype(F32)
                pick = jnp.zeros((tokens, tokens), F32)
                weigh = jnp.zeros((tokens, tokens), F32)
                m = mst.at[s % side, s // side]
                for j in range(m.shape[0] // 3):
                    top = m.shape[0] // 3
                    hit = (m[j:j + 1, :] == expert) & (m[top + j:top + j + 1, :] == off)
                    pick = jnp.where(hit, 1.0, pick)
                    weigh = jnp.where(hit, m[2 * top + j:2 * top + j + 1, :], weigh)
                sel[s] = pick[:local * WINDOW].astype(BF16)
                cst[...] = weigh.T.astype(BF16)
                out = pltpu.make_async_copy(cst, cmb_ref.at[s], csem)
                out.start()
                out.wait()

    for kc in range(6, chunks):
        shared_piece(kc)
    for j in range(3):
        tile(0, j).start()
    finish(0, tokens, hs_ref)

    @pl.loop(0, local * rows // 16)
    def _(r):
        e = r // (rows // 16)
        acc[e, pl.ds(pl.multiple_of(r % (rows // 16) * 16, 16), 16)] = jnp.zeros((16, 2 * width), F32)

    def source(c, s, half):
        o, i = (s % side, s // side) if half == 0 else (s // side, s % side)
        slot = s % 4
        return pltpu.make_async_copy(g_ref.at[c, half, o, i], xs.at[slot, half], xsem.at[slot, half])

    @pl.loop(6, chunks + 6)
    def _(t):
        @pl.when(t < chunks)
        def _():
            start(t, 0)

        @pl.when(t - 1 < chunks)
        def _():
            landed(t - 1, 0)
            start(t - 1, 1)

        @pl.when(t - 2 < chunks)
        def _():
            landed(t - 2, 1)
            for half in range(2):
                own(t - 2, half).wait()
            start(t - 2, 2)

        @pl.when(t - 4 < chunks)
        def _():
            landed(t - 4, 2)
            start(t - 4, 3)

        c = t - 6
        landed(c, 3)
        for s in range(3):
            for half in range(2):
                source(c, s, half).start()

        @pl.loop(0, n)
        def _(s):
            for half in range(2):
                source(c, s, half).wait()

            @pl.when(s + 3 < n)
            def _():
                for half in range(2):
                    source(c, s + 3, half).start()

            for half in range(2):
                cols = pl.ds(half * HALF, HALF)
                r = jnp.dot(sel[s], xs[s % 4, half], preferred_element_type=F32).astype(BF16)
                base = window_of(s, slots)
                for e in range(local):
                    old = z[e, pl.ds(base, 16), cols]
                    new = r[e * WINDOW:(e + 1) * WINDOW]
                    z[e, pl.ds(base, 16), cols] = jnp.where(s > 0, old, jnp.zeros_like(old)) + new[:16]
                    z[e, pl.ds(pl.multiple_of(base + 16, 16), WINDOW - 16), cols] = new[16:]

        for j in range(2 * local):
            e, m = j // 2, j % 2
            tile(c, j).wait()

            @pl.loop(0, width // HALF)
            def _(nb):
                cols = pl.ds(pl.multiple_of(nb * HALF, HALF), HALF)
                into = pl.ds(pl.multiple_of(m * width + nb * HALF, HALF), HALF)
                acc[e, :, into] += jnp.dot(z[e, :rows], wbuf[j % 3, :, cols], preferred_element_type=F32)

            if j + 3 < 2 * local:
                tile(c, j + 3).start()
            else:
                @pl.when(c + 1 < chunks)
                def _():
                    tile(c + 1, j + 3 - 2 * local).start()

    for e in range(local):
        finish(e, rows, h_ref.at[e])

    for k in range(6):
        meta(k).wait_send()

    @pl.loop(0, chunks)
    def _(c):
        for step in range(4):
            each(c, step, lambda cp: cp.wait_send())


def down_kernel(side, slots, h_ref, hs_ref, cmb_ref, wd_ref, sd_ref,
                y_ref, r1, r2, r3, r4,
                hv, hs, cv, wbuf, out, shc, v1, v2, v3, v4, b1, b2, b3, b4, total, yst,
                snd, rcv, wsem, vsem, ysem, lsem):
    me, pos, first, second = place(side)
    tokens = hs_ref.shape[0]
    chunks = y_ref.shape[1] // CHUNK
    local, rows = h_ref.shape[:2]
    half_rows, half_side = tokens // 2, side // 2
    landing, held, sending = (r1, r2, r3, r4), (v1, v2, v3, v4), (b1, b2, b3, b4)
    depth = out.shape[0]

    def key(step, half, di):
        return step * 4 + half * 2 + di

    def hop(c, step, half, di):
        k = key(step, half, di)
        return pltpu.make_async_remote_copy(
            src_ref=sending[step].at[c % 2, half, di], dst_ref=landing[step].at[c, half, di],
            send_sem=snd.at[c, k], recv_sem=rcv.at[c, k],
            device_id=(second if step < 2 else first)(half, DIRS[di]), device_id_type=MESH)

    def fetch(c, step, half, di):
        k = key(step, half, di)
        return pltpu.make_async_copy(landing[step].at[c, half, di], held[step].at[half, di], vsem.at[k])

    def each(act):
        for half in range(2):
            for di in range(2):
                act(half, di)

    def free(c, step):
        @pl.when(c >= 2)
        def _():
            each(lambda half, di: hop(c - 2, step, half, di).wait_send())

    def send(c, step):
        each(lambda half, di: hop(c, step, half, di).start())

    def tile(c, j):
        cols = pl.ds(pl.multiple_of(c * CHUNK, CHUNK), CHUNK)
        src = wd_ref.at[j, :, cols] if j < local else sd_ref.at[:, cols]
        return pltpu.make_async_copy(src, wbuf.at[j % 2], wsem.at[j % 2])

    def term(c, half, o, i):
        s = i * side + o if half == 0 else o * side + i
        base = window_of(s, slots)
        cols = pl.ds(half * HALF, HALF)
        parts = [out[c % depth, e, pl.ds(base, WINDOW), cols] for e in range(local)]
        parts.append(jnp.zeros((tokens - local * WINDOW, HALF), BF16))
        return jnp.dot(cv[s], jnp.concatenate(parts, axis=0), preferred_element_type=F32)

    loads = [pltpu.make_async_copy(h_ref, hv, lsem.at[0]), pltpu.make_async_copy(hs_ref, hs, lsem.at[1]),
             pltpu.make_async_copy(cmb_ref, cv, lsem.at[2])]
    for cp in loads:
        cp.start()
    for j in range(2):
        tile(0, j).start()
    for b in range(depth):
        for e in range(local):
            out[b, e, rows:] = jnp.zeros((out.shape[2] - rows, CHUNK), BF16)
    meet(side)
    for cp in loads:
        cp.wait()

    def y_put(c, half):
        cols = pl.ds(pl.multiple_of(c * CHUNK + half * HALF, HALF), HALF)
        return pltpu.make_async_copy(yst.at[c % 2, half], y_ref.at[:, cols], ysem.at[c % 2, half])

    @pl.loop(0, chunks + 8)
    def _(t):
        for step in range(4):
            c = t - 2 * (step + 1)

            @pl.when((c >= 0) & (c < chunks))
            def _():
                each(lambda half, di: hop(c, step, half, di).wait_recv())
                each(lambda half, di: fetch(c, step, half, di).start())

        @pl.when(t < chunks)
        def _():
            c = t
            for j in range(local + 1):
                tile(c, j).wait()

                @pl.loop(0, 2)
                def _(nb):
                    cols = pl.ds(pl.multiple_of(nb * HALF, HALF), HALF)
                    if j < local:
                        out[c % depth, j, :rows, cols] = jnp.dot(
                            hv[j], wbuf[j % 2, :, cols], preferred_element_type=F32).astype(BF16)
                    else:
                        shc[c, :, cols] = jnp.dot(hs[...], wbuf[j % 2, :, cols], preferred_element_type=F32)

                if j + 2 <= local:
                    tile(c, j + 2).start()
                else:
                    @pl.when(c + 1 < chunks)
                    def _():
                        tile(c + 1, j + 1 - local).start()

            free(c, 0)
            for half in range(2):
                o, i = pos[half]
                for di in range(2):
                    @pl.loop(0, half_side)
                    def _(b):
                        b1[c % 2, half, di, b] = term(c, half, (o + 2) % side, di * half_side + b).astype(BF16)
            send(c, 0)

        @pl.when((t >= 2) & (t - 2 < chunks))
        def _():
            c = t - 2
            each(lambda half, di: fetch(c, 0, half, di).wait())
            free(c, 1)
            for half in range(2):
                o, i = pos[half]
                for di in range(2):
                    to = (o + DIRS[di] + side) % side

                    @pl.loop(0, half_side)
                    def _(b):
                        own = term(c, half, to, di * half_side + b)
                        b2[c % 2, half, di, di * half_side + b] = (own + v1[half, di, b].astype(F32)).astype(BF16)
                        other = (1 - di) * half_side + b
                        b2[c % 2, half, di, other] = term(c, half, to, other).astype(BF16)
            send(c, 1)

        @pl.when((t >= 4) & (t - 4 < chunks))
        def _():
            c = t - 4
            each(lambda half, di: fetch(c, 1, half, di).wait())
            free(c, 2)
            for half in range(2):
                o, i = pos[half]
                for turn in (2, 1, 3, 0):
                    to = (i + turn) % side
                    s = term(c, half, o, to) + v2[half, 0, to].astype(F32) + v2[half, 1, to].astype(F32)
                    if turn == 2:
                        for di in range(2):
                            b3[c % 2, half, di] = s[di * half_rows:(di + 1) * half_rows].astype(BF16)
                    else:
                        total[c % depth, half, min(turn, 2)] = s
            send(c, 2)

        @pl.when((t >= 6) & (t - 6 < chunks))
        def _():
            c = t - 6
            each(lambda half, di: fetch(c, 2, half, di).wait())
            free(c, 3)
            for half in range(2):
                for di in range(2):
                    mine = pl.ds(di * half_rows, half_rows)
                    rest = pl.ds((1 - di) * half_rows, half_rows)
                    b4[c % 2, half, di, mine] = (
                        total[c % depth, half, 1 + di, mine] + v3[half, di].astype(F32)).astype(BF16)
                    b4[c % 2, half, di, rest] = total[c % depth, half, 1 + di, rest].astype(BF16)
            send(c, 3)

        @pl.when(t >= 8)
        def _():
            c = t - 8
            each(lambda half, di: fetch(c, 3, half, di).wait())

            @pl.when(c >= 2)
            def _():
                for half in range(2):
                    y_put(c - 2, half).wait()

            for half in range(2):
                s = total[c % depth, half, 0] + v4[half, 0].astype(F32) + v4[half, 1].astype(F32)
                yst[c % 2, half] = (s + shc[c, :, half * HALF:(half + 1) * HALF]).astype(BF16)
                y_put(c, half).start()

    for c in range(max(chunks - 2, 0), chunks):
        for step in range(4):
            each(lambda half, di: hop(c, step, half, di).wait_send())
        for half in range(2):
            y_put(c, half).wait()


def solution(mesh):
    n = mesh.shape["ep"]
    side = math.isqrt(n)

    def body(x, expert, slot, gate, w_gate, w_up, w_down, s_gate, s_up, s_down):
        x, expert, slot, gate = (v[0, 0] for v in (x, expert, slot, gate))
        tokens, depth = x.shape
        top = expert.shape[1]
        local, _, width = w_gate.shape
        slots = 5 * tokens * top // (4 * local * n)
        chunks = depth // CHUNK
        rows = slots * n
        padded = (slots * (n - 1)) // 16 * 16 + WINDOW
        meta = jnp.concatenate([
            expert.T.astype(F32),
            jnp.where(slot < slots, slot, -1024).T.astype(F32),
            gate.T.astype(BF16).astype(F32),
        ], axis=0)
        dma = pltpu.SemaphoreType.DMA
        h, hs, cmb, _, _ = pl.pallas_call(
            functools.partial(up_kernel, side, slots),
            out_shape=(
                jax.ShapeDtypeStruct((local, rows, width), BF16),
                jax.ShapeDtypeStruct((tokens, width), BF16),
                jax.ShapeDtypeStruct((n, tokens, tokens), BF16),
                jax.ShapeDtypeStruct((chunks, 2, side, side, tokens, HALF), BF16),
                jax.ShapeDtypeStruct((side, side, *meta.shape), F32),
            ),
            in_specs=[ANY] * 6,
            out_specs=(ANY,) * 5,
            scratch_shapes=[
                pltpu.VMEM((local, rows, 2 * width), F32),
                pltpu.VMEM((local, padded, CHUNK), BF16),
                pltpu.VMEM((4, 2, tokens, HALF), BF16),
                pltpu.VMEM((tokens, depth), BF16),
                pltpu.VMEM((3, CHUNK, width), BF16),
                pltpu.VMEM((n, local * WINDOW, tokens), BF16),
                pltpu.VMEM((side, side, *meta.shape), F32),
                pltpu.VMEM((2, rows, HALF), BF16),
                pltpu.VMEM((tokens, tokens), BF16),
                dma((chunks, 16)), dma((chunks, 16)), dma((6,)), dma((6,)), dma((3,)), dma((4, 2)),
                dma((chunks, 2)), dma((2,)), dma(()), dma((2,)),
            ],
            compiler_params=pltpu.CompilerParams(
                collective_id=0, has_side_effects=True, vmem_limit_bytes=67043328),
            name="dispatch_up",
        )(x, meta, w_gate, w_up, s_gate, s_up)
        y = pl.pallas_call(
            functools.partial(down_kernel, side, slots),
            out_shape=(
                jax.ShapeDtypeStruct((tokens, depth), BF16),
                jax.ShapeDtypeStruct((chunks, 2, 2, side // 2, tokens, HALF), BF16),
                jax.ShapeDtypeStruct((chunks, 2, 2, side, tokens, HALF), BF16),
                jax.ShapeDtypeStruct((chunks, 2, 2, tokens // 2, HALF), BF16),
                jax.ShapeDtypeStruct((chunks, 2, 2, tokens, HALF), BF16),
            ),
            in_specs=[ANY] * 5,
            out_specs=(ANY,) * 5,
            scratch_shapes=[
                pltpu.VMEM((local, rows, width), BF16),
                pltpu.VMEM((tokens, width), BF16),
                pltpu.VMEM((n, tokens, tokens), BF16),
                pltpu.VMEM((2, width, CHUNK), BF16),
                pltpu.VMEM((5, local, padded, CHUNK), BF16),
                pltpu.VMEM((chunks, tokens, CHUNK), F32),
                pltpu.VMEM((2, 2, side // 2, tokens, HALF), BF16),
                pltpu.VMEM((2, 2, side, tokens, HALF), BF16),
                pltpu.VMEM((2, 2, tokens // 2, HALF), BF16),
                pltpu.VMEM((2, 2, tokens, HALF), BF16),
                pltpu.VMEM((2, 2, 2, side // 2, tokens, HALF), BF16),
                pltpu.VMEM((2, 2, 2, side, tokens, HALF), BF16),
                pltpu.VMEM((2, 2, 2, tokens // 2, HALF), BF16),
                pltpu.VMEM((2, 2, 2, tokens, HALF), BF16),
                pltpu.VMEM((5, 2, 3, tokens, HALF), F32),
                pltpu.VMEM((2, 2, tokens, HALF), BF16),
                dma((chunks, 16)), dma((chunks, 16)), dma((2,)), dma((16,)), dma((2, 2)), dma((3,)),
            ],
            compiler_params=pltpu.CompilerParams(
                collective_id=1, has_side_effects=True, vmem_limit_bytes=67043328),
            name="down_combine",
        )(h, hs, cmb, w_down, s_down)[0]
        return y[None, None]

    token, expert, whole = P("dp", "ep", None, None), P("ep", None, None), P(None, None)
    return jax.shard_map(
        body,
        mesh=mesh,
        in_specs=(token,) * 4 + (expert,) * 3 + (whole,) * 3,
        out_specs=token,
        check_vma=False,
    )
```

```python
import functools
import math

import jax
import jax.numpy as jnp
from jax import lax
from jax.experimental import pallas as pl
from jax.experimental.pallas import tpu as pltpu
from jax.sharding import PartitionSpec as P

MESH = pl.DeviceIdType.MESH
F32, BF16 = jnp.float32, jnp.bfloat16
ANY = pl.BlockSpec(memory_space=pl.ANY)
DIRS = (1, -1)
HALF = 256
CHUNK = 2 * HALF
WIDE = 1024
WINDOW = 80


def place(side):
    me = lax.axis_index("ep")
    x, y = me // side, me % side

    def at(dx, dy):
        return {"ep": (x + dx + side) % side * side + (y + dy + side) % side}

    def first(half, d):
        return at(d, 0) if half == 0 else at(0, d)

    def second(half, d):
        return at(0, d) if half == 0 else at(d, 0)

    return me, ((y, x), (x, y)), first, second


def meet(side):
    _, _, first, second = place(side)
    barrier = pltpu.get_barrier_semaphore()
    for d in DIRS:
        pl.semaphore_signal(barrier, inc=1, device_id=first(0, d), device_id_type=MESH)
        pl.semaphore_signal(barrier, inc=1, device_id=second(0, d), device_id_type=MESH)
    pl.semaphore_wait(barrier, 4)


def window_of(s, slots):
    return pl.multiple_of(slots * s // 16 * 16, 16)


def up_kernel(side, slots, x_ref, meta_ref, wg_ref, wu_ref, sg_ref, su_ref,
              h_ref, hs_ref, cmb_ref, g_ref, gm_ref,
              acc, z, xs, xown, wbuf, sel, mst, hst, cst,
              snd, rcv, msnd, mrcv, wsem, xsem, osem, hsem, csem, lsem):
    me, pos, first, second = place(side)
    n = side * side
    tokens, depth = x_ref.shape
    width = wg_ref.shape[2]
    chunks = depth // CHUNK
    local = wg_ref.shape[0]
    rows = slots * n

    def gather(c, step, half, di):
        d = DIRS[di]
        o, i = pos[half]
        k = step * 4 + half * 2 + di
        part = pl.ds(0 if di == 0 else tokens // 2, tokens // 2)
        pair = pl.ds(0 if di == 0 else side // 2, side // 2)
        if step == 0:
            src = xown.at[:, pl.ds(pl.multiple_of(c * CHUNK + half * HALF, HALF), HALF)]
            dst = g_ref.at[c, half, o, i]
        elif step == 1:
            src = dst = g_ref.at[c, half, o, (i - d + side) % side, part]
        elif step == 2:
            src = dst = g_ref.at[c, half, o]
        else:
            src = dst = g_ref.at[c, half, (o - d + side) % side, pair]
        return pltpu.make_async_remote_copy(
            src_ref=src, dst_ref=dst, send_sem=snd.at[c, k], recv_sem=rcv.at[c, k],
            device_id=(first if step < 2 else second)(half, d), device_id_type=MESH)

    def each(c, step, act):
        for half in range(2):
            for di in range(2):
                act(gather(c, step, half, di))

    def start(c, step):
        each(c, step, lambda cp: cp.start())

    def landed(c, step):
        each(c, step, lambda cp: cp.wait_recv())

    y, x = pos[0]

    def meta(k):
        di = k % 2
        d = DIRS[di]
        if k < 2:
            src, dst, to = meta_ref, gm_ref.at[y, x], first(0, d)
        elif k == 2:
            src = dst = gm_ref.at[y, (x - 1 + side) % side]
            to = first(0, 1)
        elif k < 5:
            src = dst = gm_ref.at[y]
            to = second(0, DIRS[k - 3])
        else:
            src = dst = gm_ref.at[(y - 1 + side) % side]
            to = second(0, 1)
        return pltpu.make_async_remote_copy(
            src_ref=src, dst_ref=dst, send_sem=msnd.at[k], recv_sem=mrcv.at[k],
            device_id=to, device_id_type=MESH)

    def own(c, half):
        o, i = pos[half]
        return pltpu.make_async_copy(
            xown.at[:, pl.ds(pl.multiple_of(c * CHUNK + half * HALF, HALF), HALF)],
            g_ref.at[c, half, o, i], osem.at[c, half])

    def shared_tile(q):
        ref = (sg_ref, su_ref)[q % 2]
        return pltpu.make_async_copy(ref.at[pl.ds(q // 2 * CHUNK, CHUNK)], wbuf.at[q % 3], wsem.at[q % 3])

    def tile(c, e, m):
        slot = (2 * e + m) % 3
        ref = (wg_ref, wu_ref)[m]
        return pltpu.make_async_copy(
            ref.at[e, pl.ds(pl.multiple_of(c * CHUNK, CHUNK), CHUNK)], wbuf.at[slot], wsem.at[slot])

    load_x = pltpu.make_async_copy(x_ref, xown, lsem.at[0])
    load_x.start()
    keep_meta = pltpu.make_async_copy(meta_ref, mst.at[y, x], lsem.at[1])
    keep_meta.start()
    for q in range(3):
        shared_tile(q).start()
    meet(side)
    load_x.wait()
    keep_meta.wait()
    put_meta = pltpu.make_async_copy(mst.at[y, x], gm_ref.at[y, x], lsem.at[1])
    put_meta.start()

    for k in range(2):
        meta(k).start()

    @pl.loop(0, chunks)
    def _(c):
        for half in range(2):
            own(c, half).start()

    def shared_piece(kc):
        for m in range(2):
            q = kc * 2 + m
            shared_tile(q).wait()

            @pl.loop(0, width // WIDE)
            def _(nb):
                cols = pl.ds(pl.multiple_of(nb * WIDE, WIDE), WIDE)
                into = pl.ds(pl.multiple_of(m * width + nb * WIDE, WIDE), WIDE)
                r = jnp.dot(xown[:, kc * CHUNK:(kc + 1) * CHUNK], wbuf[q % 3, :, cols], preferred_element_type=F32)
                if kc > 0:
                    r = acc[0, :tokens, into] + r
                acc[0, :tokens, into] = r

            if q + 3 < 2 * chunks:
                shared_tile(q + 3).start()

    def finish(e, m_rows, dst_ref):
        def put(b, slot):
            cols = pl.ds(pl.multiple_of(b * HALF, HALF), HALF)
            return pltpu.make_async_copy(hst.at[slot, pl.ds(0, m_rows)], dst_ref.at[:, cols], hsem.at[slot])

        for b in range(width // HALF):
            slot = b % 2
            if b >= 2:
                put(b - 2, slot).wait()
            cols = pl.ds(b * HALF, HALF)
            ups = pl.ds(width + b * HALF, HALF)
            gate = acc[e, :m_rows, cols]
            hst[slot, :m_rows] = (jax.nn.silu(gate) * acc[e, :m_rows, ups]).astype(BF16)
            put(b, slot).start()
        for b in range(width // HALF - 2, width // HALF):
            put(b, b % 2).wait()

    def exchange(t, at):
        at(t, lambda c: start(c, 0))

        def second_step(c):
            landed(c, 0)
            start(c, 1)

        def third_step(c):
            landed(c, 1)
            for half in range(2):
                own(c, half).wait()
            start(c, 2)

        def fourth_step(c):
            landed(c, 2)
            start(c, 3)

        at(t - 1, second_step)
        at(t - 5, fourth_step)
        at(t - 3, third_step)

    def if_static(c, act):
        if 0 <= c < chunks:
            act(c)

    def if_traced(c, act):
        pl.when(c < chunks)(lambda: act(c))

    for t in range(6):
        if t == 1:
            for k in range(2):
                meta(k).wait_recv()
            meta(2).start()
        if t == 2:
            put_meta.wait()
            meta(2).wait_recv()
            meta(3).start()
            meta(4).start()
        if t == 3:
            meta(3).wait_recv()
            meta(4).wait_recv()
            meta(5).start()
        exchange(t, if_static)
        shared_piece(t)

    meta(5).wait_recv()
    load_m = pltpu.make_async_copy(gm_ref, mst, lsem.at[1])
    load_m.start()
    load_m.wait()

    def put_weights(s):
        return pltpu.make_async_copy(cst.at[s % 2], cmb_ref.at[s], csem.at[s % 2])

    @pl.loop(0, n)
    def _(s):
        r = lax.broadcasted_iota(jnp.int32, (tokens, 1), 0)
        e = (r >= WINDOW).astype(jnp.int32) + (r >= 2 * WINDOW).astype(jnp.int32)
        off = (r - e * WINDOW + window_of(s, slots) - slots * s).astype(F32)
        expert = jnp.where(r < local * WINDOW, me * local + e, -1).astype(F32)
        pick = jnp.zeros((tokens, tokens), F32)
        weigh = jnp.zeros((tokens, tokens), F32)
        m = mst.at[s % side, s // side]
        top = m.shape[0] // 3
        for j in range(top):
            hit = (m[j:j + 1, :] == expert) & (m[top + j:top + j + 1, :] == off)
            pick = jnp.where(hit, 1.0, pick)
            weigh = jnp.where(hit, m[2 * top + j:2 * top + j + 1, :], weigh)
        sel[s] = pick[:local * WINDOW].astype(BF16)

        @pl.when(s >= 2)
        def _():
            put_weights(s - 2).wait()

        cst[s % 2] = weigh.T.astype(BF16)
        put_weights(s).start()

    for s in range(n - 2, n):
        put_weights(s).wait()

    for kc in range(6, chunks):
        shared_piece(kc)
    for j in range(3):
        tile(0, j // 2, j % 2).start()
    finish(0, tokens, hs_ref)

    @pl.loop(0, local * rows // 16)
    def _(r):
        e = r // (rows // 16)
        acc[e, pl.ds(pl.multiple_of(r % (rows // 16) * 16, 16), 16)] = jnp.zeros((16, 2 * width), F32)

    def source(c, q, half):
        src = g_ref.at[c, half, :, q] if half == 0 else g_ref.at[c, half, q]
        return pltpu.make_async_copy(src, xs.at[q, half], xsem.at[q, half])

    @pl.loop(6, chunks + 6)
    def _(t):
        exchange(t, if_traced)
        c = t - 6
        landed(c, 3)
        for q in range(side):
            for half in range(2):
                source(c, q, half).start()

        @pl.loop(0, side)
        def _(q):
            for half in range(2):
                source(c, q, half).wait()

            for half in range(2):
                cols = pl.ds(half * HALF, HALF)
                for b in range(side):
                    s = q * side + b
                    r = jnp.dot(sel[s], xs[q, half, b], preferred_element_type=F32).astype(BF16)
                    base = window_of(s, slots)
                    for e in range(local):
                        new = r[e * WINDOW:(e + 1) * WINDOW]
                        old = z[e, pl.ds(base, 16), cols]
                        if b == 0:
                            old = jnp.where(q > 0, old, jnp.zeros_like(old))
                        z[e, pl.ds(base, 16), cols] = old + new[:16]
                        z[e, pl.ds(pl.multiple_of(base + 16, 16), WINDOW - 16), cols] = new[16:]

        @pl.loop(0, local)
        def _(e):
            for m in range(2):
                slot = (2 * e + m) % 3
                tile(c, e, m).wait()

                @pl.loop(0, width // WIDE)
                def _(nb):
                    cols = pl.ds(pl.multiple_of(nb * WIDE, WIDE), WIDE)
                    into = pl.ds(pl.multiple_of(m * width + nb * WIDE, WIDE), WIDE)
                    acc[e, :, into] += jnp.dot(z[e, :rows], wbuf[slot, :, cols], preferred_element_type=F32)

                later = e + 1 + m

                @pl.when(later < local)
                def _():
                    tile(c, later, 1 - m).start()

                @pl.when((later >= local) & (c + 1 < chunks))
                def _():
                    tile(c + 1, later - local, 1 - m).start()

    for e in range(local):
        finish(e, rows, h_ref.at[e])

    for k in range(6):
        meta(k).wait_send()

    @pl.loop(0, chunks)
    def _(c):
        for step in range(4):
            each(c, step, lambda cp: cp.wait_send())


def down_kernel(side, slots, h_ref, hs_ref, cmb_ref, wd_ref, sd_ref,
                y_ref, r1, r2, r3, r4,
                hv, hs, cv, wbuf, out, shc, v1, v2, v3, v4, b1, b2, b3, b4, total, yst,
                snd, rcv, wsem, vsem, ysem, lsem):
    me, pos, first, second = place(side)
    tokens = hs_ref.shape[0]
    chunks = y_ref.shape[1] // CHUNK
    local, rows = h_ref.shape[:2]
    half_rows, half_side = tokens // 2, side // 2
    landing, held, sending = (r1, r2, r3, r4), (v1, v2, v3, v4), (b1, b2, b3, b4)
    depth = out.shape[0]

    def key(step, half, di):
        return step * 4 + half * 2 + di

    def hop(c, step, half, di):
        k = key(step, half, di)
        return pltpu.make_async_remote_copy(
            src_ref=sending[step].at[c % 2, half, di], dst_ref=landing[step].at[c, half, di],
            send_sem=snd.at[c, k], recv_sem=rcv.at[c, k],
            device_id=(second if step < 2 else first)(half, DIRS[di]), device_id_type=MESH)

    def fetch(c, step, half, di):
        k = key(step, half, di)
        return pltpu.make_async_copy(landing[step].at[c, half, di], held[step].at[half, di], vsem.at[k])

    def each(act):
        for half in range(2):
            for di in range(2):
                act(half, di)

    def free(c, step):
        @pl.when(c >= 2)
        def _():
            each(lambda half, di: hop(c - 2, step, half, di).wait_send())

    def send(c, step):
        each(lambda half, di: hop(c, step, half, di).start())

    def tile(c, j):
        cols = pl.ds(pl.multiple_of(c * CHUNK, CHUNK), CHUNK)
        src = wd_ref.at[j, :, cols] if j < local else sd_ref.at[:, cols]
        return pltpu.make_async_copy(src, wbuf.at[j % 2], wsem.at[j % 2])

    def term(c, half, o, i):
        s = i * side + o if half == 0 else o * side + i
        base = window_of(s, slots)
        cols = pl.ds(half * HALF, HALF)
        parts = [out[c % depth, e, pl.ds(base, WINDOW), cols] for e in range(local)]
        parts.append(jnp.zeros((tokens - local * WINDOW, HALF), BF16))
        return jnp.dot(cv[s], jnp.concatenate(parts, axis=0), preferred_element_type=F32)

    loads = [pltpu.make_async_copy(h_ref.at[e], hv.at[e], lsem.at[e]) for e in range(local)]
    loads += [pltpu.make_async_copy(hs_ref, hs, lsem.at[local]), pltpu.make_async_copy(cmb_ref, cv, lsem.at[local + 1])]
    loads[0].start()
    for j in range(2):
        tile(0, j).start()
    for cp in loads[1:]:
        cp.start()
    for b in range(depth):
        for e in range(local):
            out[b, e, rows:] = jnp.zeros((out.shape[2] - rows, CHUNK), BF16)
    meet(side)

    def y_put(c, half):
        cols = pl.ds(pl.multiple_of(c * CHUNK + half * HALF, HALF), HALF)
        return pltpu.make_async_copy(yst.at[c % 2, half], y_ref.at[:, cols], ysem.at[c % 2, half])

    @pl.loop(0, chunks + 7)
    def _(t):
        for step in range(1, 4):
            c = t - 2 * step - 1

            @pl.when((c >= 0) & (c < chunks))
            def _():
                each(lambda half, di: hop(c, step, half, di).wait_recv())
                each(lambda half, di: fetch(c, step, half, di).start())

        @pl.when(t < chunks)
        def _():
            c = t
            for j in range(local + 1):
                tile(c, j).wait()

                @pl.when(c == 0)
                def _():
                    loads[j].wait()

                @pl.loop(0, 2)
                def _(nb):
                    cols = pl.ds(pl.multiple_of(nb * HALF, HALF), HALF)
                    if j < local:
                        out[c % depth, j, :rows, cols] = jnp.dot(
                            hv[j], wbuf[j % 2, :, cols], preferred_element_type=F32).astype(BF16)
                    else:
                        shc[c, :, cols] = jnp.dot(hs[...], wbuf[j % 2, :, cols], preferred_element_type=F32)

                if j + 2 <= local:
                    tile(c, j + 2).start()
                else:
                    @pl.when(c + 1 < chunks)
                    def _():
                        tile(c + 1, j + 1 - local).start()

        @pl.when((t >= 1) & (t - 1 < chunks))
        def _():
            each(lambda half, di: hop(t - 1, 0, half, di).wait_recv())
            each(lambda half, di: fetch(t - 1, 0, half, di).start())

        @pl.when(t < chunks)
        def _():
            c = t

            @pl.when(c == 0)
            def _():
                loads[local + 1].wait()

            free(c, 0)
            for half in range(2):
                o, i = pos[half]
                for di in range(2):
                    @pl.loop(0, half_side)
                    def _(b):
                        b1[c % 2, half, di, b] = term(c, half, (o + 2) % side, di * half_side + b).astype(BF16)
            send(c, 0)

        @pl.when((t >= 1) & (t - 1 < chunks))
        def _():
            c = t - 1
            each(lambda half, di: fetch(c, 0, half, di).wait())
            free(c, 1)
            for half in range(2):
                o, i = pos[half]
                for di in range(2):
                    to = (o + DIRS[di] + side) % side

                    @pl.loop(0, half_side)
                    def _(b):
                        own = term(c, half, to, di * half_side + b)
                        b2[c % 2, half, di, di * half_side + b] = (own + v1[half, di, b].astype(F32)).astype(BF16)
                        other = (1 - di) * half_side + b
                        b2[c % 2, half, di, other] = term(c, half, to, other).astype(BF16)
            send(c, 1)

        @pl.when((t >= 3) & (t - 3 < chunks))
        def _():
            c = t - 3
            each(lambda half, di: fetch(c, 1, half, di).wait())
            free(c, 2)
            for half in range(2):
                o, i = pos[half]
                for turn in (2, 1, 3, 0):
                    to = (i + turn) % side
                    s = term(c, half, o, to) + v2[half, 0, to].astype(F32) + v2[half, 1, to].astype(F32)
                    if turn == 2:
                        for di in range(2):
                            b3[c % 2, half, di] = s[di * half_rows:(di + 1) * half_rows].astype(BF16)
                    else:
                        total[c % depth, half, min(turn, 2)] = s
            send(c, 2)

        @pl.when((t >= 5) & (t - 5 < chunks))
        def _():
            c = t - 5
            each(lambda half, di: fetch(c, 2, half, di).wait())
            free(c, 3)
            for half in range(2):
                for di in range(2):
                    mine = pl.ds(di * half_rows, half_rows)
                    rest = pl.ds((1 - di) * half_rows, half_rows)
                    b4[c % 2, half, di, mine] = (
                        total[c % depth, half, 1 + di, mine] + v3[half, di].astype(F32)).astype(BF16)
                    b4[c % 2, half, di, rest] = total[c % depth, half, 1 + di, rest].astype(BF16)
            send(c, 3)

        @pl.when(t >= 7)
        def _():
            c = t - 7
            each(lambda half, di: fetch(c, 3, half, di).wait())

            @pl.when(c >= 2)
            def _():
                for half in range(2):
                    y_put(c - 2, half).wait()

            for half in range(2):
                s = total[c % depth, half, 0] + v4[half, 0].astype(F32) + v4[half, 1].astype(F32)
                yst[c % 2, half] = (s + shc[c, :, half * HALF:(half + 1) * HALF]).astype(BF16)
                y_put(c, half).start()

    for c in range(max(chunks - 2, 0), chunks):
        for step in range(4):
            each(lambda half, di: hop(c, step, half, di).wait_send())
        for half in range(2):
            y_put(c, half).wait()


def solution(mesh):
    n = mesh.shape["ep"]
    side = math.isqrt(n)

    def body(x, expert, slot, gate, w_gate, w_up, w_down, s_gate, s_up, s_down):
        x, expert, slot, gate = (v[0, 0] for v in (x, expert, slot, gate))
        tokens, depth = x.shape
        top = expert.shape[1]
        local, _, width = w_gate.shape
        slots = 5 * tokens * top // (4 * local * n)
        chunks = depth // CHUNK
        rows = slots * n
        padded = (slots * (n - 1)) // 16 * 16 + WINDOW
        meta = jnp.concatenate([
            expert.T.astype(F32),
            jnp.where(slot < slots, slot, -1024).T.astype(F32),
            gate.T.astype(BF16).astype(F32),
        ], axis=0)
        dma = pltpu.SemaphoreType.DMA
        h, hs, cmb, _, _ = pl.pallas_call(
            functools.partial(up_kernel, side, slots),
            out_shape=(
                jax.ShapeDtypeStruct((local, rows, width), BF16),
                jax.ShapeDtypeStruct((tokens, width), BF16),
                jax.ShapeDtypeStruct((n, tokens, tokens), BF16),
                jax.ShapeDtypeStruct((chunks, 2, side, side, tokens, HALF), BF16),
                jax.ShapeDtypeStruct((side, side, *meta.shape), F32),
            ),
            in_specs=[ANY] * 6,
            out_specs=(ANY,) * 5,
            scratch_shapes=[
                pltpu.VMEM((local, rows, 2 * width), F32),
                pltpu.VMEM((local, padded, CHUNK), BF16),
                pltpu.VMEM((side, 2, side, tokens, HALF), BF16),
                pltpu.VMEM((tokens, depth), BF16),
                pltpu.VMEM((3, CHUNK, width), BF16),
                pltpu.VMEM((n, local * WINDOW, tokens), BF16),
                pltpu.VMEM((side, side, *meta.shape), F32),
                pltpu.VMEM((2, rows, HALF), BF16),
                pltpu.VMEM((2, tokens, tokens), BF16),
                dma((chunks, 16)), dma((chunks, 16)), dma((6,)), dma((6,)), dma((3,)), dma((side, 2)),
                dma((chunks, 2)), dma((2,)), dma((2,)), dma((2,)),
            ],
            compiler_params=pltpu.CompilerParams(
                collective_id=0, has_side_effects=True, vmem_limit_bytes=67043328),
            name="dispatch_up",
        )(x, meta, w_gate, w_up, s_gate, s_up)
        y = pl.pallas_call(
            functools.partial(down_kernel, side, slots),
            out_shape=(
                jax.ShapeDtypeStruct((tokens, depth), BF16),
                jax.ShapeDtypeStruct((chunks, 2, 2, side // 2, tokens, HALF), BF16),
                jax.ShapeDtypeStruct((chunks, 2, 2, side, tokens, HALF), BF16),
                jax.ShapeDtypeStruct((chunks, 2, 2, tokens // 2, HALF), BF16),
                jax.ShapeDtypeStruct((chunks, 2, 2, tokens, HALF), BF16),
            ),
            in_specs=[ANY] * 5,
            out_specs=(ANY,) * 5,
            scratch_shapes=[
                pltpu.VMEM((local, rows, width), BF16),
                pltpu.VMEM((tokens, width), BF16),
                pltpu.VMEM((n, tokens, tokens), BF16),
                pltpu.VMEM((2, width, CHUNK), BF16),
                pltpu.VMEM((5, local, padded, CHUNK), BF16),
                pltpu.VMEM((chunks, tokens, CHUNK), F32),
                pltpu.VMEM((2, 2, side // 2, tokens, HALF), BF16),
                pltpu.VMEM((2, 2, side, tokens, HALF), BF16),
                pltpu.VMEM((2, 2, tokens // 2, HALF), BF16),
                pltpu.VMEM((2, 2, tokens, HALF), BF16),
                pltpu.VMEM((2, 2, 2, side // 2, tokens, HALF), BF16),
                pltpu.VMEM((2, 2, 2, side, tokens, HALF), BF16),
                pltpu.VMEM((2, 2, 2, tokens // 2, HALF), BF16),
                pltpu.VMEM((2, 2, 2, tokens, HALF), BF16),
                pltpu.VMEM((5, 2, 3, tokens, HALF), F32),
                pltpu.VMEM((2, 2, tokens, HALF), BF16),
                dma((chunks, 16)), dma((chunks, 16)), dma((2,)), dma((16,)), dma((2, 2)), dma((local + 2,)),
            ],
            compiler_params=pltpu.CompilerParams(
                collective_id=1, has_side_effects=True, vmem_limit_bytes=67043328),
            name="down_combine",
        )(h, hs, cmb, w_down, s_down)[0]
        return y[None, None]

    token, expert, whole = P("dp", "ep", None, None), P("ep", None, None), P(None, None)
    return jax.shard_map(
        body,
        mesh=mesh,
        in_specs=(token,) * 4 + (expert,) * 3 + (whole,) * 3,
        out_specs=token,
        check_vma=False,
    )
```
